32 devices in a mesh: group: 2 (over y), space: 8 (over z, x), tm: 2 (over core).
Axes of the slice: x: 2, y: 2, z: 4, core: 2. Of those that a mesh axis runs over, the one named last changes fastest.
Arguments:
- w_modes: bfloat16 [12, 1024, 768], P(('group', 'tm'), 'space'), parts along dimension 0, may hold values from -6 to 6
- v_modes: bfloat16 [12, 1024, 768], P(('group', 'tm'), 'space'), parts along dimension 0, may hold values from -6 to 6
- phase_index: int32 [1024], P('space'), may hold values from 0 to 95
- seq_offset: int32 [6], replicated, may hold values from 1 to 5
- owner_block: int32 [8], replicated, may hold values from 0 to 7, each once
Outputs:
- strips: float32 [384, 12, 768], P('space', ('group', 'tm')), parts along dimension 1
- margin: float32 [12, 768], P(('group', 'tm')), parts along dimension 0
The draws below stay inside these ranges and needn't reach their ends.
There are 2 independent parts, one for each index of `group`. The reference program is written for one: setup_inputs(seed, part) draws one part's arguments, and reference() takes and returns one part's arrays. A program takes and returns all parts, laid end to end along the dimension named above; an argument that names none is the same for every part. Nothing has to cross between parts.
Inputs may be any that keep to these rules, and one draw needn't show every extreme that they name: owner_block is a permutation of 0 to 7.
All inputs are finite; a program needn't handle non-finite values.
Results may differ from the reference program's by a relative error of at most 0.0041.
Values may be sent and summed in bfloat16 or wider, within the bound.
No kernel may reach another device: no remote copies, remote signals or barrier semaphores. Data moves between devices by JAX's collectives and lax.ppermute only.
A program may use at most 64 MiB of HBM per device.

```python
import math
import jax
import jax.numpy as jnp
from jax import lax

NMODE = 384
MAXOFF = 5
PHASES = 96
NT = 6
SITES = 1024
OWNERS = 8
N_SPACE = 8


def touch_ends(array, own_key, least, largest):
    longest = array.shape.index(max(array.shape))
    spots = []
    for shift in (0, 1):
        where = [jax.random.randint(jax.random.fold_in(own_key, axis), (), 0, length) for axis, length in enumerate(array.shape)]
        where[longest] = (where[longest] + shift) % array.shape[longest]
        spots.append(tuple(where))
    return array.at[spots[0]].set(least).at[spots[1]].set(largest)


def shard_levels(stream_key, dims, cuts, low, high):
    gain, own = 1.0, jax.random.fold_in(stream_key, 6)
    for axis_at, parts in cuts:
        heights = jnp.exp(jax.random.uniform(jax.random.fold_in(own, axis_at), (parts,), jnp.float32, low / len(cuts), high / len(cuts)))
        gain = gain * jnp.repeat(heights, dims[axis_at] // parts).reshape([-1 if axis == axis_at else 1 for axis in range(len(dims))])
    return gain


def centred(own_key, shape, spread, reach, pieces=(), held_as=jnp.bfloat16):
    level = shard_levels(own_key, shape, pieces, -0.22, 0.18) if pieces else 1.0
    array = jax.random.normal(own_key, shape, jnp.float32) * spread * level
    return jnp.minimum(jnp.maximum(array, -reach), reach).astype(held_as)


def setup_inputs(seed: int = 0, part: int = 0) -> dict:
    key_list = jax.random.split(jax.random.key(seed), 6)
    part_splits = jax.random.split(jax.random.fold_in(key_list[5], part), 6)
    w_modes = centred(part_splits[0], (NT, SITES, 2 * NMODE), 1.0, 6.0, ((0, 2), (1, 8)))
    v_modes = centred(part_splits[1], (NT, SITES, 2 * NMODE), 1.0, 6.0, ((0, 2), (1, 8)))
    phase_index = touch_ends(jax.random.randint(key_list[2], (SITES,), 0, PHASES), jax.random.fold_in(key_list[2], 1), 0, PHASES - 1).astype(jnp.int32)
    seq_offset = touch_ends(jax.random.randint(key_list[3], (NT,), 1, MAXOFF + 1), jax.random.fold_in(key_list[3], 1), 1, MAXOFF).astype(jnp.int32)
    owner_block = jax.random.permutation(key_list[4], OWNERS).astype(jnp.int32)
    return {"w_modes": w_modes, "v_modes": v_modes, "phase_index": phase_index, "seq_offset": seq_offset, "owner_block": owner_block}


def reference(w_modes, v_modes, phase_index, seq_offset, owner_block):
    block = NMODE // N_SPACE
    scale_sites = 1.0 / math.sqrt(SITES)
    scale_modes = 1.0 / math.sqrt(2 * NMODE)
    angle = phase_index.astype(jnp.float32) * (2.0 * math.pi / PHASES)
    cosv = jnp.cos(angle)[:, None]
    sinv = jnp.sin(angle)[:, None]

    def margin_slice(pair):
        w_slice, v_slice = pair
        v_real = v_slice[:, :NMODE].astype(jnp.float32)
        v_imag = v_slice[:, NMODE:].astype(jnp.float32)
        ph_real = (cosv * v_real + sinv * v_imag).astype(jnp.bfloat16)
        ph_imag = (cosv * v_imag - sinv * v_real).astype(jnp.bfloat16)
        left = jnp.concatenate([w_slice[:, :NMODE], w_slice[:, NMODE:]], axis=0)
        right = jnp.concatenate([jnp.concatenate([ph_real, ph_imag], axis=1), jnp.concatenate([ph_imag, -ph_real], axis=1)], axis=0)
        return jnp.dot(left.T, right, preferred_element_type=jnp.float32) * scale_sites
    fields = lax.map(margin_slice, (w_modes, v_modes))
    order = (owner_block[:, None] * block + jnp.arange(block, dtype=jnp.int32)[None, :]).reshape(-1).astype(jnp.int32)
    strips = jnp.transpose(jnp.take(fields, order, axis=1), (1, 0, 2))
    rounded = fields.astype(jnp.bfloat16)
    times = jnp.arange(NT, dtype=jnp.int32)
    target = ((times + seq_offset) % NT).astype(jnp.int32)
    chosen = jnp.take(rounded, target, axis=0)

    def second_slice(triple):
        w_slice, v_slice, matrix = triple
        v_two = jnp.concatenate([jnp.concatenate([v_slice[:, :NMODE], -v_slice[:, NMODE:]], axis=1), jnp.concatenate([v_slice[:, NMODE:], v_slice[:, :NMODE]], axis=1)], axis=0)
        seq = jnp.dot(v_two, matrix.T, preferred_element_type=jnp.float32) * scale_modes
        seq_real = seq[:SITES]
        seq_imag = seq[SITES:]
        w_real = w_slice[:, :NMODE].astype(jnp.float32)
        w_imag = w_slice[:, NMODE:].astype(jnp.float32)
        over_real = lax.optimization_barrier(jnp.sum(w_real * seq_real + w_imag * seq_imag, axis=0))
        over_imag = lax.optimization_barrier(jnp.sum(w_real * seq_imag - w_imag * seq_real, axis=0))
        return jnp.concatenate([over_real, over_imag]) * scale_sites
    margin = lax.map(second_slice, (w_modes, v_modes, chosen))
    return (strips, margin)
```

```python
import functools
import math

import jax
import jax.numpy as jnp
from jax import lax
from jax.experimental import pallas as pl
from jax.experimental.pallas import tpu as pltpu
from jax.sharding import PartitionSpec as P

PHASES = 96
LANES = 128


def swap(block, axis, mask):
    size = lax.axis_size(axis)
    return lax.ppermute(block, axis, [(i, i ^ mask) for i in range(size)])


def estimate(flops, moved):
    return pl.CostEstimate(flops=flops, bytes_accessed=moved, transcendentals=0)


def prep_kernel(nline, block, owner_ref, w_ref, v_ref, send_ref, own_ref, turned):
    width = w_ref.shape[2]
    nmode = width // 2
    me = lax.axis_index("space")
    line, side = me // 2, me % 2
    for c in range(width // LANES):
        turned[c * LANES : (c + 1) * LANES, :] = w_ref[0, :, c * LANES : (c + 1) * LANES].T
    for k in range(nline):
        for half, out_ref in ((1 - side, send_ref), (side, own_ref)):
            rows = owner_ref[2 * (line ^ k) + half] * block
            for part in range(2):
                at = (part * nline + k) * block
                out_ref[at : at + block, :] = turned[pl.ds(pl.multiple_of(part * nmode + rows, block), block), :]
    base, sites = 2 * nline * block, v_ref.shape[1]
    for c in range(width // LANES):
        send_ref[base + c * sites : base + (c + 1) * sites, :] = v_ref[0, :, c * LANES : (c + 1) * LANES]


def field_kernel(nline, block, scale, cs_ref, v_ref, own_ref, got_ref, *refs):
    outs, (left, phased, plain) = refs[:-3], refs[-3:]
    sites, width = v_ref.shape[1:]
    nmode = width // 2
    rows = nline * block
    base = 2 * rows
    for part in range(2):
        at = 2 * part * sites
        left[:, at : at + sites] = own_ref[part * rows : (part + 1) * rows, :]
        left[:, at + sites : at + 2 * sites] = got_ref[part * rows : (part + 1) * rows, :]
    for c in range(nmode // LANES):
        re, im = slice(c * LANES, (c + 1) * LANES), slice(nmode + c * LANES, nmode + (c + 1) * LANES)
        far = c + nmode // LANES
        for d in range(2):
            if d == 0:
                vr, vi = v_ref[0, :, re], v_ref[0, :, im]
            else:
                vr = got_ref[base + c * sites : base + (c + 1) * sites, :]
                vi = got_ref[base + far * sites : base + (far + 1) * sites, :]
            top, low = slice(d * sites, (d + 1) * sites), slice((2 + d) * sites, (3 + d) * sites)
            plain[top, re], plain[top, im] = vr, vi
            plain[low, re], plain[low, im] = vi, -vr
            cosv, sinv = cs_ref[:, 2 * d : 2 * d + 1], cs_ref[:, 2 * d + 1 : 2 * d + 2]
            fr, fi = vr.astype(jnp.float32), vi.astype(jnp.float32)
            pr = (cosv * fr + sinv * fi).astype(jnp.bfloat16)
            pi = (cosv * fi - sinv * fr).astype(jnp.bfloat16)
            phased[top, re], phased[top, im] = pr, pi
            phased[low, re], phased[low, im] = pi, -pr
    for which, right in enumerate((phased, plain)):
        field = jnp.dot(left[...], right[...], preferred_element_type=jnp.float32) * scale
        for k in range(nline):
            outs[k][which] = field[k * block : (k + 1) * block].astype(outs[k].dtype)


def strip_kernel(tdev, nline, *refs):
    ins, (strip_ref, round_ref) = refs[:-2], refs[-2:]
    for t in range(tdev):
        total = ins[t * nline][0]
        for k in range(1, nline):
            total = total + ins[t * nline + k][0].astype(jnp.float32)
        strip_ref[:, t, :] = total
        round_ref[t] = total.astype(jnp.bfloat16)


def margin_kernel(tdev, nline, scale, pick_ref, owner_ref, mine_ref, other_ref, *refs):
    ins, out_ref = refs[:-1], refs[-1]
    block, width = mine_ref.shape[1:]
    nmode = width // 2
    first = owner_ref[lax.axis_index("space")] * block
    lane = lax.broadcasted_iota(jnp.int32, (block, nmode), 1)
    row = lax.broadcasted_iota(jnp.int32, (block, nmode), 0)
    here = lane == row + first
    for t in range(tdev):
        total = ins[t * nline][1]
        for k in range(1, nline):
            total = total + ins[t * nline + k][1].astype(jnp.float32)
        pick = pick_ref[t]
        near = pick < tdev
        at = jnp.where(near, pick, pick - tdev)
        matrix = jnp.where(near, mine_ref[at], other_ref[at]).astype(jnp.float32)
        mr, mi = matrix[:, :nmode], matrix[:, nmode:]
        gr, gi = total[:, :nmode], total[:, nmode:]
        real = jnp.sum(mr * gr - mi * gi, axis=1, keepdims=True) * scale
        imag = jnp.sum(mr * gi + mi * gr, axis=1, keepdims=True) * scale
        out_ref[t : t + 1, :nmode] = jnp.sum(jnp.where(here, real, 0.0), axis=0, keepdims=True)
        out_ref[t : t + 1, nmode:] = jnp.sum(jnp.where(here, imag, 0.0), axis=0, keepdims=True)


def aligned_shards(w_modes, v_modes, phase_index, seq_offset, owner_block):
    tdev, sdev, width = w_modes.shape
    nmode = width // 2
    nspace, ntm = lax.axis_size("space"), lax.axis_size("tm")
    block, nline = nmode // nspace, nspace // 2
    total_slices = tdev * ntm
    scale_sites = 1.0 / math.sqrt(sdev * nspace)
    scale_modes = 1.0 / math.sqrt(2 * nmode)
    rows = nline * block
    bf16, f32 = jnp.bfloat16, jnp.float32
    vmem, smem = pl.BlockSpec(memory_space=pltpu.VMEM), pl.BlockSpec(memory_space=pltpu.SMEM)

    other_phase = swap(phase_index, "space", 1)
    sends, owns = [], []
    for t in range(tdev):
        slice_spec = pl.BlockSpec((1, sdev, width), lambda i, t=t: (t, 0, 0))
        send, own = pl.pallas_call(
            functools.partial(prep_kernel, nline, block),
            grid=(1,),
            out_shape=(
                jax.ShapeDtypeStruct((2 * rows + width // LANES * sdev, LANES), bf16),
                jax.ShapeDtypeStruct((2 * rows, LANES), bf16),
            ),
            in_specs=[smem, slice_spec, slice_spec],
            out_specs=(vmem, vmem),
            scratch_shapes=[pltpu.VMEM((width, LANES), bf16)],
            cost_estimate=estimate(2_000_000, 4 * sdev * width * 2),
            name=f"prep_{t}",
        )(owner_block, w_modes, v_modes)
        sends.append(send)
        owns.append(own)
    gots = [swap(send, "space", 1) for send in sends]

    angle = jnp.stack([phase_index, other_phase], axis=1).astype(f32) * (2.0 * math.pi / PHASES)
    cosv, sinv = jnp.cos(angle), jnp.sin(angle)
    cs = jnp.stack([cosv[:, 0], sinv[:, 0], cosv[:, 1], sinv[:, 1]], axis=1)

    parts = []
    for t in range(tdev):
        outs = pl.pallas_call(
            functools.partial(field_kernel, nline, block, scale_sites),
            grid=(1,),
            out_shape=[jax.ShapeDtypeStruct((2, block, width), f32 if k == 0 else bf16) for k in range(nline)],
            in_specs=[vmem, pl.BlockSpec((1, sdev, width), lambda i, t=t: (t, 0, 0)), vmem, vmem],
            out_specs=[vmem] * nline,
            scratch_shapes=[
                pltpu.VMEM((rows, 4 * sdev), bf16),
                pltpu.VMEM((4 * sdev, width), bf16),
                pltpu.VMEM((4 * sdev, width), bf16),
            ],
            cost_estimate=estimate(4 * rows * 4 * sdev * width, 8 * sdev * width),
            name=f"field_{t}",
        )(cs, v_modes, owns[t], gots[t])
        parts.append(outs[0])
        parts.extend(swap(outs[k], "space", 2 * k) for k in range(1, nline))

    strips, rounded = pl.pallas_call(
        functools.partial(strip_kernel, tdev, nline),
        out_shape=(jax.ShapeDtypeStruct((block, tdev, width), f32), jax.ShapeDtypeStruct((tdev, block, width), bf16)),
        in_specs=[vmem] * len(parts),
        out_specs=(vmem, vmem),
        cost_estimate=estimate(1_000_000, tdev * block * width * 20),
        name="strip",
    )(*parts)
    other = swap(rounded, "tm", 1)

    rank = lax.axis_index("tm")
    global_slice = rank * tdev + jnp.arange(tdev, dtype=jnp.int32)
    target = (global_slice + jnp.take(seq_offset, global_slice)) % total_slices
    pick = (target - rank * tdev) % total_slices
    margin = pl.pallas_call(
        functools.partial(margin_kernel, tdev, nline, scale_sites_of_margin(scale_modes)),
        out_shape=jax.ShapeDtypeStruct((tdev, width), f32),
        in_specs=[smem, smem, vmem, vmem] + [vmem] * len(parts),
        out_specs=vmem,
        cost_estimate=estimate(2_000_000, tdev * block * width * 20),
        name="margin",
    )(pick, owner_block, rounded, other, *parts)
    mask = 1
    while mask < nspace:
        margin = margin + swap(margin, "space", mask)
        mask *= 2
    return strips, margin


def scale_sites_of_margin(scale_modes):
    return scale_modes


def general_shards(w_modes, v_modes, phase_index, seq_offset, owner_block):
    tdev, sdev, width = w_modes.shape
    nmode = width // 2
    nspace = lax.axis_size("space")
    ntm = lax.axis_size("tm")
    block = nmode // nspace
    total_slices = tdev * ntm
    scale_sites = 1.0 / math.sqrt(sdev * nspace)
    scale_modes = 1.0 / math.sqrt(2 * nmode)
    order = (owner_block[:, None] * block + jnp.arange(block, dtype=jnp.int32)[None, :]).reshape(-1)
    w_real = jnp.take(w_modes[:, :, :nmode], order, axis=2)
    w_imag = jnp.take(w_modes[:, :, nmode:], order, axis=2)
    left = jnp.concatenate([w_real, w_imag], axis=1)
    angle = phase_index.astype(jnp.float32) * (2.0 * math.pi / PHASES)
    cosv = jnp.cos(angle)[None, :, None]
    sinv = jnp.sin(angle)[None, :, None]
    v_real = v_modes[:, :, :nmode].astype(jnp.float32)
    v_imag = v_modes[:, :, nmode:].astype(jnp.float32)
    ph_real = (cosv * v_real + sinv * v_imag).astype(jnp.bfloat16)
    ph_imag = (cosv * v_imag - sinv * v_real).astype(jnp.bfloat16)
    right = jnp.concatenate(
        [jnp.concatenate([ph_real, ph_imag], axis=2), jnp.concatenate([ph_imag, -ph_real], axis=2)],
        axis=1,
    )
    rank = lax.axis_index("tm")
    global_slice = rank * tdev + jnp.arange(tdev, dtype=jnp.int32)
    target = (global_slice + jnp.take(seq_offset, global_slice)) % total_slices
    pick = (target - rank * tdev) % total_slices
    v_two = jnp.concatenate(
        [
            jnp.concatenate([v_modes[:, :, :nmode], -v_modes[:, :, nmode:]], axis=2),
            jnp.concatenate([v_modes[:, :, nmode:], v_modes[:, :, :nmode]], axis=2),
        ],
        axis=1,
    )
    full = lax.psum(
        jnp.einsum("tsi,tsj->itj", left, right, preferred_element_type=jnp.float32) * scale_sites,
        "space",
    )
    strips = lax.dynamic_slice_in_dim(full, lax.axis_index("space") * block, block, 0)
    rounded = full.astype(jnp.bfloat16)
    pieces = [rounded]
    for step in range(1, ntm):
        route = [((i + step) % ntm, i) for i in range(ntm)]
        pieces.append(lax.ppermute(rounded, "tm", route))
    chosen = jnp.take(jnp.concatenate(pieces, axis=1), pick, axis=1)
    seq_raw = jnp.einsum("tsj,itj->tsi", v_two, chosen, preferred_element_type=jnp.float32)
    seq = seq_raw * scale_modes
    seq_real = seq[:, :sdev]
    seq_imag = seq[:, sdev:]
    wr_full = w_real.astype(jnp.float32)
    wi_full = w_imag.astype(jnp.float32)
    over_real = jnp.sum(wr_full * seq_real + wi_full * seq_imag, axis=1) * scale_sites
    over_imag = jnp.sum(wr_full * seq_imag - wi_full * seq_real, axis=1) * scale_sites
    total_real, total_imag = lax.psum((over_real, over_imag), "space")
    margin = jnp.zeros((tdev, 2 * nmode), jnp.float32)
    margin = margin.at[:, order].set(total_real).at[:, order + nmode].set(total_imag)
    return (strips, margin)


def shards(w_modes, v_modes, phase_index, seq_offset, owner_block):
    _, sdev, width = w_modes.shape
    nmode, nspace = width // 2, lax.axis_size("space")
    power = nspace >= 4 and nspace & (nspace - 1) == 0
    tiles = nmode % (nspace * 16) == 0 and nmode % LANES == 0 and sdev == LANES
    body = aligned_shards if power and tiles and lax.axis_size("tm") == 2 else general_shards
    return body(w_modes, v_modes, phase_index, seq_offset, owner_block)


def solution(mesh):
    in_specs = (
        P(("group", "tm"), "space", None),
        P(("group", "tm"), "space", None),
        P("space"),
        P(),
        P(),
    )
    out_specs = (P("space", ("group", "tm"), None), P(("group", "tm"), None))
    return jax.shard_map(shards, mesh=mesh, in_specs=in_specs, out_specs=out_specs, check_vma=False)
```

```python
import functools
import math

import jax
import jax.numpy as jnp
from jax import lax
from jax.experimental import pallas as pl
from jax.experimental.pallas import tpu as pltpu
from jax.sharding import PartitionSpec as P


PHASES = 96
LANES = 128
GRANT = 12 * 1024 * 1024


def swap(block, axis, mask):
    size = lax.axis_size(axis)
    return lax.ppermute(block, axis, [(i, i ^ mask) for i in range(size)])


PHASE_ROWS = 16


def prep_kernel(t, nline, block, owner_ref, phase_ref, w_ref, v_ref, send_ref, own_ref, turned):
    width = w_ref.shape[2]
    nmode = width // 2
    me = lax.axis_index("space")
    line, side = me // 2, me % 2
    for c in range(width // LANES):
        turned[c * LANES : (c + 1) * LANES, :] = w_ref[t, :, c * LANES : (c + 1) * LANES].T
    for k in range(nline):
        for half, out_ref in ((1 - side, send_ref), (side, own_ref)):
            rows = owner_ref[2 * (line ^ k) + half] * block
            for part in range(2):
                at = (part * nline + k) * block
                out_ref[at : at + block, :] = turned[pl.ds(pl.multiple_of(part * nmode + rows, block), block), :]
    base, sites = 2 * nline * block, v_ref.shape[1]
    for c in range(width // LANES):
        send_ref[base + c * sites : base + (c + 1) * sites, :] = v_ref[t, :, c * LANES : (c + 1) * LANES]
    base += width // LANES * sites
    phase = phase_ref[...].astype(jnp.float32).astype(jnp.bfloat16)
    send_ref[base : base + PHASE_ROWS, :] = jnp.broadcast_to(phase, (PHASE_ROWS, LANES))


def field_kernel(t, nline, block, scale, phase_ref, v_ref, own_ref, got_ref, *refs):
    (mine_ref, near_ref), far_refs, (left, phased, plain) = refs[:2], refs[2:-3], refs[-3:]
    sites, width = v_ref.shape[1:]
    nmode = width // 2
    rows = nline * block
    base = 2 * rows
    tail = base + width // LANES * sites
    for part in range(2):
        at = 2 * part * sites
        left[:, at : at + sites] = own_ref[part * rows : (part + 1) * rows, :]
        left[:, at + sites : at + 2 * sites] = got_ref[part * rows : (part + 1) * rows, :]
    theirs = got_ref[tail : tail + PHASE_ROWS, :].astype(jnp.float32)[:1]
    angle = jnp.concatenate([phase_ref[...].astype(jnp.float32), theirs], axis=0) * (2.0 * math.pi / PHASES)
    turns = jnp.concatenate([jnp.cos(angle), jnp.sin(angle), jnp.zeros((4, LANES), jnp.float32)], axis=0).T
    for c in range(nmode // LANES):
        re, im = slice(c * LANES, (c + 1) * LANES), slice(nmode + c * LANES, nmode + (c + 1) * LANES)
        far = c + nmode // LANES
        for d in range(2):
            if d == 0:
                vr, vi = v_ref[t, :, re], v_ref[t, :, im]
            else:
                vr = got_ref[base + c * sites : base + (c + 1) * sites, :]
                vi = got_ref[base + far * sites : base + (far + 1) * sites, :]
            top, low = slice(d * sites, (d + 1) * sites), slice((2 + d) * sites, (3 + d) * sites)
            plain[top, re], plain[top, im] = vr, vi
            plain[low, re], plain[low, im] = vi, -vr
            cosv, sinv = turns[:, d : d + 1], turns[:, 2 + d : 3 + d]
            fr, fi = vr.astype(jnp.float32), vi.astype(jnp.float32)
            pr = (cosv * fr + sinv * fi).astype(jnp.bfloat16)
            pi = (cosv * fi - sinv * fr).astype(jnp.bfloat16)
            phased[top, re], phased[top, im] = pr, pi
            phased[low, re], phased[low, im] = pi, -pr

    def part_of(field, k):
        return field[k * block : (k + 1) * block]

    field = jnp.dot(left[...], phased[...], preferred_element_type=jnp.float32) * scale
    mine_ref[0] = part_of(field, 0)
    near_ref[0] = part_of(field, 1).astype(jnp.bfloat16)
    for k in range(2, nline):
        far_refs[k - 2][...] = part_of(field, k).astype(jnp.bfloat16)
    field = jnp.dot(left[...], plain[...], preferred_element_type=jnp.float32) * scale
    for k in range(nline):
        if k % 2 == 0:
            mine_ref[1 + k // 2] = part_of(field, k)
        else:
            near_ref[1 + k // 2] = part_of(field, k).astype(jnp.bfloat16)


def cross_kernel(mine_ref, near_ref, out_ref):
    out_ref[...] = (mine_ref[2] + near_ref[2].astype(jnp.float32)).astype(jnp.bfloat16)


def strip_kernel(tdev, *refs):
    ins, (strip_ref, round_ref) = refs[:-2], refs[-2:]
    each = len(ins) // tdev
    for t in range(tdev):
        mine_ref, near_ref, *far_refs = ins[t * each : (t + 1) * each]
        total = mine_ref[0] + near_ref[0].astype(jnp.float32)
        for far_ref in far_refs:
            total = total + far_ref[...].astype(jnp.float32)
        strip_ref[t] = total
        round_ref[t] = total.astype(jnp.bfloat16)


def margin_kernel(tdev, scale, pick_ref, owner_ref, rounded_ref, other_ref, *refs):
    ins, out_ref = refs[:-1], refs[-1]
    block, width = rounded_ref.shape[1:]
    nmode = width // 2
    first = owner_ref[lax.axis_index("space")] * block
    lane = lax.broadcasted_iota(jnp.int32, (block, nmode), 1)
    row = lax.broadcasted_iota(jnp.int32, (block, nmode), 0)
    here = lane == row + first
    for t in range(tdev):
        mine_ref, near_ref, cross_ref = ins[3 * t : 3 * t + 3]
        total = mine_ref[1] + near_ref[1].astype(jnp.float32) + cross_ref[...].astype(jnp.float32)
        pick = pick_ref[t]
        inside = pick < tdev
        at = jnp.where(inside, pick, pick - tdev)
        matrix = jnp.where(inside, rounded_ref[at], other_ref[at]).astype(jnp.float32)
        mr, mi = matrix[:, :nmode], matrix[:, nmode:]
        gr, gi = total[:, :nmode], total[:, nmode:]
        real = jnp.sum(mr * gr - mi * gi, axis=1, keepdims=True) * scale
        imag = jnp.sum(mr * gi + mi * gr, axis=1, keepdims=True) * scale
        out_ref[t : t + 1, :nmode] = jnp.sum(jnp.where(here, real, 0.0), axis=0, keepdims=True)
        out_ref[t : t + 1, nmode:] = jnp.sum(jnp.where(here, imag, 0.0), axis=0, keepdims=True)


def aligned_shards(w_modes, v_modes, phase_index, seq_offset, owner_block):
    tdev, sdev, width = w_modes.shape
    nmode = width // 2
    nspace, ntm = lax.axis_size("space"), lax.axis_size("tm")
    block, nline = nmode // nspace, nspace // 2
    total_slices = tdev * ntm
    scale_sites = 1.0 / math.sqrt(sdev * nspace)
    scale_modes = 1.0 / math.sqrt(2 * nmode)
    rows = nline * block
    bf16, f32 = jnp.bfloat16, jnp.float32
    vmem, smem = pl.BlockSpec(memory_space=pltpu.VMEM), pl.BlockSpec(memory_space=pltpu.SMEM)
    shape = jax.ShapeDtypeStruct

    def call(kernel, outs, n_scalar, cost, args, scratch=()):
        return pl.pallas_call(
            kernel,
            out_shape=outs,
            in_specs=[smem] * n_scalar + [vmem] * (len(args) - n_scalar),
            out_specs=jax.tree.map(lambda _: vmem, outs),
            scratch_shapes=scratch,
            compiler_params=pltpu.CompilerParams(vmem_limit_bytes=GRANT),
            cost_estimate=pl.CostEstimate(flops=cost, bytes_accessed=1_000_000, transcendentals=0),
        )(*args)

    phases = phase_index.reshape(1, sdev)
    packed = 2 * rows + width // LANES * sdev + PHASE_ROWS
    sends, owns = [], []
    for t in range(tdev):
        send, own = call(
            functools.partial(prep_kernel, t, nline, block),
            (shape((packed, LANES), bf16), shape((2 * rows, LANES), bf16)),
            1,
            4_000_000,
            (owner_block, phases, w_modes, v_modes),
            [pltpu.VMEM((width, LANES), bf16)],
        )
        sends.append(send)
        owns.append(own)
    gots = [swap(send, "space", 1) for send in sends]

    fields, sums = [], []
    for t in range(tdev):
        mine, near, *fars = call(
            functools.partial(field_kernel, t, nline, block, scale_sites),
            [shape((3, block, width), f32), shape((3, block, width), bf16)] + [shape((block, width), bf16)] * (nline - 2),
            0,
            4 * rows * 4 * sdev * width,
            (phases, v_modes, owns[t], gots[t]),
            [pltpu.VMEM((rows, 4 * sdev), bf16)] + [pltpu.VMEM((4 * sdev, width), bf16)] * 2,
        )
        near = swap(near, "space", 2)
        fars = [swap(far, "space", 2 * k) for k, far in enumerate(fars, 2)]
        cross = call(cross_kernel, shape((block, width), bf16), 0, 1_000_000, (mine, near))
        fields.extend([mine, near, *fars])
        sums.extend([mine, near, swap(cross, "space", 4)])

    strips, rounded = call(
        functools.partial(strip_kernel, tdev),
        (shape((tdev, block, width), f32), shape((tdev, block, width), bf16)),
        0,
        1_000_000,
        fields,
    )
    other = swap(rounded, "tm", 1)

    rank = lax.axis_index("tm")
    global_slice = rank * tdev + jnp.arange(tdev, dtype=jnp.int32)
    target = (global_slice + jnp.take(seq_offset, global_slice)) % total_slices
    pick = (target - rank * tdev) % total_slices
    margin = call(
        functools.partial(margin_kernel, tdev, scale_modes),
        shape((tdev, width), f32),
        2,
        1_000_000,
        (pick, owner_block, rounded, other, *sums),
    )
    mask = 1
    while mask < nspace:
        margin = margin + swap(margin, "space", mask)
        mask *= 2
    return jnp.transpose(strips, (1, 0, 2)), margin


def general_shards(w_modes, v_modes, phase_index, seq_offset, owner_block):
    tdev, sdev, width = w_modes.shape
    nmode = width // 2
    nspace = lax.axis_size("space")
    ntm = lax.axis_size("tm")
    block = nmode // nspace
    total_slices = tdev * ntm
    scale_sites = 1.0 / math.sqrt(sdev * nspace)
    scale_modes = 1.0 / math.sqrt(2 * nmode)
    order = (owner_block[:, None] * block + jnp.arange(block, dtype=jnp.int32)[None, :]).reshape(-1)
    w_real = jnp.take(w_modes[:, :, :nmode], order, axis=2)
    w_imag = jnp.take(w_modes[:, :, nmode:], order, axis=2)
    left = jnp.concatenate([w_real, w_imag], axis=1)
    angle = phase_index.astype(jnp.float32) * (2.0 * math.pi / PHASES)
    cosv = jnp.cos(angle)[None, :, None]
    sinv = jnp.sin(angle)[None, :, None]
    v_real = v_modes[:, :, :nmode].astype(jnp.float32)
    v_imag = v_modes[:, :, nmode:].astype(jnp.float32)
    ph_real = (cosv * v_real + sinv * v_imag).astype(jnp.bfloat16)
    ph_imag = (cosv * v_imag - sinv * v_real).astype(jnp.bfloat16)
    right = jnp.concatenate(
        [jnp.concatenate([ph_real, ph_imag], axis=2), jnp.concatenate([ph_imag, -ph_real], axis=2)],
        axis=1,
    )
    rank = lax.axis_index("tm")
    global_slice = rank * tdev + jnp.arange(tdev, dtype=jnp.int32)
    target = (global_slice + jnp.take(seq_offset, global_slice)) % total_slices
    pick = (target - rank * tdev) % total_slices
    v_two = jnp.concatenate(
        [
            jnp.concatenate([v_modes[:, :, :nmode], -v_modes[:, :, nmode:]], axis=2),
            jnp.concatenate([v_modes[:, :, nmode:], v_modes[:, :, :nmode]], axis=2),
        ],
        axis=1,
    )
    full = lax.psum(
        jnp.einsum("tsi,tsj->itj", left, right, preferred_element_type=jnp.float32) * scale_sites,
        "space",
    )
    strips = lax.dynamic_slice_in_dim(full, lax.axis_index("space") * block, block, 0)
    rounded = full.astype(jnp.bfloat16)
    pieces = [rounded]
    for step in range(1, ntm):
        route = [((i + step) % ntm, i) for i in range(ntm)]
        pieces.append(lax.ppermute(rounded, "tm", route))
    chosen = jnp.take(jnp.concatenate(pieces, axis=1), pick, axis=1)
    seq_raw = jnp.einsum("tsj,itj->tsi", v_two, chosen, preferred_element_type=jnp.float32)
    seq = seq_raw * scale_modes
    seq_real = seq[:, :sdev]
    seq_imag = seq[:, sdev:]
    wr_full = w_real.astype(jnp.float32)
    wi_full = w_imag.astype(jnp.float32)
    over_real = jnp.sum(wr_full * seq_real + wi_full * seq_imag, axis=1) * scale_sites
    over_imag = jnp.sum(wr_full * seq_imag - wi_full * seq_real, axis=1) * scale_sites
    total_real, total_imag = lax.psum((over_real, over_imag), "space")
    margin = jnp.zeros((tdev, 2 * nmode), jnp.float32)
    margin = margin.at[:, order].set(total_real).at[:, order + nmode].set(total_imag)
    return (strips, margin)


def shards(w_modes, v_modes, phase_index, seq_offset, owner_block):
    _, sdev, width = w_modes.shape
    nmode, nspace = width // 2, lax.axis_size("space")
    square = nspace == 2 * 4
    tiles = nmode % (nspace * 16) == 0 and nmode % LANES == 0 and sdev == LANES
    body = aligned_shards if square and tiles and lax.axis_size("tm") == 2 else general_shards
    return body(w_modes, v_modes, phase_index, seq_offset, owner_block)


def solution(mesh):
    in_specs = (
        P(("group", "tm"), "space", None),
        P(("group", "tm"), "space", None),
        P("space"),
        P(),
        P(),
    )
    out_specs = (P("space", ("group", "tm"), None), P(("group", "tm"), None))
    step = jax.shard_map(shards, mesh=mesh, in_specs=in_specs, out_specs=out_specs, check_vma=False)

    def run(w_modes, *rest):
        return step(w_modes, *rest)

    return run if mesh.shape["space"] == 8 else step
```

```python
import functools
import math
from typing import NamedTuple

import jax
import jax.numpy as jnp
from jax import lax
from jax.experimental import pallas as pl
from jax.experimental.pallas import tpu as pltpu
from jax.sharding import PartitionSpec as P


PHASES = 96
LANES = 128
GRANT = 12 * 1024 * 1024


def swap(block, axis, mask):
    size = lax.axis_size(axis)
    return lax.ppermute(block, axis, [(i, i ^ mask) for i in range(size)])


class Route(NamedTuple):
    pair: int
    near: int
    over: int
    halve_phased: bool

    def masks(self):
        return (0, self.near, self.over, self.near | self.over)


def routes(slices):
    along_x, along_z = Route(1, 2, 4, False), Route(2, 1, 4, True)
    return [along_z if t % 3 == 1 else along_x for t in range(slices)]


PHASE_ROWS = 16


def pack(route, block, owner_ref, w_ref, phase_ref, send_ref, own_ref, turned):
    width = w_ref.shape[-1]
    nmode = width // 2
    me = lax.axis_index("space")
    masks = route.masks()
    nline = len(masks)
    for c in range(width // LANES):
        turned[c * LANES : (c + 1) * LANES, :] = w_ref[:, c * LANES : (c + 1) * LANES].T
    for k, mask in enumerate(masks):
        for out_ref, whose in ((send_ref, me ^ route.pair), (own_ref, me)):
            rows = owner_ref[whose ^ mask] * block
            for part in range(2):
                at = (part * nline + k) * block
                out_ref[at : at + block, :] = turned[pl.ds(pl.multiple_of(part * nmode + rows, block), block), :]
    phase = phase_ref[...].astype(jnp.float32).astype(jnp.bfloat16)
    send_ref[send_ref.shape[0] - PHASE_ROWS :, :] = jnp.broadcast_to(phase, (PHASE_ROWS, LANES))


def first_prep_kernel(t, route, block, owner_any, phase_any, w_any, v_any, send_ref, own_ref, turned, w_buf, phase_buf, owner_buf, sems):
    sites, width = w_buf.shape
    base = 2 * len(route.masks()) * block
    copies = [
        pltpu.make_async_copy(owner_any, owner_buf, sems.at[0]),
        pltpu.make_async_copy(phase_any, phase_buf, sems.at[1]),
        pltpu.make_async_copy(w_any.at[t], w_buf, sems.at[2]),
    ]
    for c in range(width // LANES):
        copies.append(
            pltpu.make_async_copy(
                v_any.at[t, :, c * LANES : (c + 1) * LANES],
                send_ref.at[base + c * sites : base + (c + 1) * sites, :],
                sems.at[3 + c],
            )
        )
    for copy in copies:
        copy.start()
    for copy in copies[:3]:
        copy.wait()
    pack(route, block, owner_buf, w_buf, phase_buf, send_ref, own_ref, turned)
    for copy in copies[3:]:
        copy.wait()


def prep_kernel(t, route, block, owner_ref, phase_ref, w_ref, v_ref, send_ref, own_ref, turned):
    sites, width = v_ref.shape[1:]
    base = 2 * len(route.masks()) * block
    for c in range(width // LANES):
        send_ref[base + c * sites : base + (c + 1) * sites, :] = v_ref[t, :, c * LANES : (c + 1) * LANES]
    pack(route, block, owner_ref, w_ref.at[t], phase_ref, send_ref, own_ref, turned)


def field_kernel(t, route, block, scale, phase_ref, v_ref, own_ref, got_ref, *refs):
    (mine_ref, near_ref), far_refs, (left, phased, plain) = refs[:2], refs[2:-3], refs[-3:]
    nline = len(route.masks())
    sites, width = v_ref.shape[1:]
    nmode = width // 2
    rows = nline * block
    base = 2 * rows
    tail = base + width // LANES * sites
    for part in range(2):
        at = 2 * part * sites
        left[:, at : at + sites] = own_ref[part * rows : (part + 1) * rows, :]
        left[:, at + sites : at + 2 * sites] = got_ref[part * rows : (part + 1) * rows, :]
    theirs = got_ref[tail : tail + PHASE_ROWS, :].astype(jnp.float32)[:1]
    angle = jnp.concatenate([phase_ref[...].astype(jnp.float32), theirs], axis=0) * (2.0 * math.pi / PHASES)
    turns = jnp.concatenate([jnp.cos(angle), jnp.sin(angle), jnp.zeros((4, LANES), jnp.float32)], axis=0).T
    for c in range(nmode // LANES):
        re, im = slice(c * LANES, (c + 1) * LANES), slice(nmode + c * LANES, nmode + (c + 1) * LANES)
        far = c + nmode // LANES
        for d in range(2):
            if d == 0:
                vr, vi = v_ref[t, :, re], v_ref[t, :, im]
            else:
                vr = got_ref[base + c * sites : base + (c + 1) * sites, :]
                vi = got_ref[base + far * sites : base + (far + 1) * sites, :]
            top, low = slice(d * sites, (d + 1) * sites), slice((2 + d) * sites, (3 + d) * sites)
            plain[top, re], plain[top, im] = vr, vi
            plain[low, re], plain[low, im] = vi, -vr
            cosv, sinv = turns[:, d : d + 1], turns[:, 2 + d : 3 + d]
            fr, fi = vr.astype(jnp.float32), vi.astype(jnp.float32)
            pr = (cosv * fr + sinv * fi).astype(jnp.bfloat16)
            pi = (cosv * fi - sinv * fr).astype(jnp.bfloat16)
            phased[top, re], phased[top, im] = pr, pi
            phased[low, re], phased[low, im] = pi, -pr

    def rows_of(field, k):
        return field[k * block : (k + 1) * block]

    slot = 0
    for right, halve in ((phased, route.halve_phased), (plain, True)):
        field = jnp.dot(left[...], right[...], preferred_element_type=jnp.float32) * scale
        mine_ref[slot] = rows_of(field, 0)
        near_ref[slot] = rows_of(field, 1).astype(jnp.bfloat16)
        slot += 1
        if halve:
            mine_ref[slot] = rows_of(field, 2)
            near_ref[slot] = rows_of(field, 3).astype(jnp.bfloat16)
            slot += 1
        else:
            for k in (2, 3):
                far_refs[k - 2][...] = rows_of(field, k).astype(jnp.bfloat16)


def cross_kernel(route, mine_ref, near_ref, out_ref):
    for i, slot in enumerate((1, 3) if route.halve_phased else (2,)):
        out_ref[i] = (mine_ref[slot] + near_ref[slot].astype(jnp.float32)).astype(jnp.bfloat16)


def strip_kernel(plan, *refs):
    ins, (strip_ref, round_ref) = list(refs[:-2]), refs[-2:]
    for t, route in enumerate(plan):
        mine_ref, near_ref = ins.pop(0), ins.pop(0)
        total = mine_ref[0] + near_ref[0].astype(jnp.float32)
        if route.halve_phased:
            total = total + ins.pop(0)[0].astype(jnp.float32)
        else:
            total = total + ins.pop(0)[...].astype(jnp.float32) + ins.pop(0)[...].astype(jnp.float32)
        strip_ref[t] = total
        round_ref[t] = total.astype(jnp.bfloat16)


def margin_kernel(plan, scale, pick_ref, owner_ref, rounded_ref, other_ref, *refs):
    ins, out_ref = refs[:-1], refs[-1]
    block, width = rounded_ref.shape[1:]
    nmode = width // 2
    first = owner_ref[lax.axis_index("space")] * block
    lane = lax.broadcasted_iota(jnp.int32, (block, nmode), 1)
    row = lax.broadcasted_iota(jnp.int32, (block, nmode), 0)
    here = lane == row + first
    tdev = len(plan)
    for t, route in enumerate(plan):
        mine_ref, near_ref, cross_ref = ins[3 * t : 3 * t + 3]
        slot, last = (2, 1) if route.halve_phased else (1, 0)
        total = mine_ref[slot] + near_ref[slot].astype(jnp.float32) + cross_ref[last].astype(jnp.float32)
        pick = pick_ref[t]
        inside = pick < tdev
        at = jnp.where(inside, pick, pick - tdev)
        matrix = jnp.where(inside, rounded_ref[at], other_ref[at]).astype(jnp.float32)
        mr, mi = matrix[:, :nmode], matrix[:, nmode:]
        gr, gi = total[:, :nmode], total[:, nmode:]
        real = jnp.sum(mr * gr - mi * gi, axis=1, keepdims=True) * scale
        imag = jnp.sum(mr * gi + mi * gr, axis=1, keepdims=True) * scale
        out_ref[t : t + 1, :nmode] = jnp.sum(jnp.where(here, real, 0.0), axis=0, keepdims=True)
        out_ref[t : t + 1, nmode:] = jnp.sum(jnp.where(here, imag, 0.0), axis=0, keepdims=True)


def aligned_shards(w_modes, v_modes, phase_index, seq_offset, owner_block):
    tdev, sdev, width = w_modes.shape
    nmode = width // 2
    nspace, ntm = lax.axis_size("space"), lax.axis_size("tm")
    block, nline = nmode // nspace, nspace // 2
    total_slices = tdev * ntm
    scale_sites = 1.0 / math.sqrt(sdev * nspace)
    scale_modes = 1.0 / math.sqrt(2 * nmode)
    rows = nline * block
    bf16, f32 = jnp.bfloat16, jnp.float32
    vmem, smem = pl.BlockSpec(memory_space=pltpu.VMEM), pl.BlockSpec(memory_space=pltpu.SMEM)
    shape = jax.ShapeDtypeStruct

    def call(kernel, outs, n_scalar, cost, args, scratch=(), specs=None):
        return pl.pallas_call(
            kernel,
            out_shape=outs,
            in_specs=specs or [smem] * n_scalar + [vmem] * (len(args) - n_scalar),
            out_specs=jax.tree.map(lambda _: vmem, outs),
            scratch_shapes=scratch,
            compiler_params=pltpu.CompilerParams(vmem_limit_bytes=GRANT),
            cost_estimate=pl.CostEstimate(flops=cost, bytes_accessed=1_000_000, transcendentals=0),
        )(*args)

    phases = phase_index.reshape(1, sdev)
    packed = 2 * rows + width // LANES * sdev + PHASE_ROWS
    plan = routes(tdev)
    sends, owns = [], []
    for t, route in enumerate(plan):
        first = t == 0
        scratch = [pltpu.VMEM((width, LANES), bf16)]
        if first:
            scratch += [
                pltpu.VMEM((sdev, width), bf16),
                pltpu.VMEM((1, sdev), jnp.int32),
                pltpu.SMEM((nspace,), jnp.int32),
                pltpu.SemaphoreType.DMA((3 + width // LANES,)),
            ]
        send, own = call(
            functools.partial(first_prep_kernel if first else prep_kernel, t, route, block),
            (shape((packed, LANES), bf16), shape((2 * rows, LANES), bf16)),
            1,
            4_000_000,
            tuple(pltpu.with_memory_space_constraint(a, pltpu.HBM) for a in (owner_block, phases, w_modes, v_modes))
            if first
            else (owner_block, phases, w_modes, v_modes),
            scratch,
            [pl.BlockSpec(memory_space=pltpu.HBM)] * 4 if first else None,
        )
        sends.append(send)
        owns.append(own)
    gots = [swap(send, "space", plan[t].pair) for t, send in enumerate(sends)]

    fields, sums = [], []
    for t, route in enumerate(plan):
        slots = 4 if route.halve_phased else 3
        mine, near, *fars = call(
            functools.partial(field_kernel, t, route, block, scale_sites),
            [shape((slots, block, width), f32), shape((slots, block, width), bf16)]
            + [shape((block, width), bf16)] * (0 if route.halve_phased else 2),
            0,
            4 * rows * 4 * sdev * width,
            (phases, v_modes, owns[t], gots[t]),
            [pltpu.VMEM((rows, 4 * sdev), bf16)] + [pltpu.VMEM((4 * sdev, width), bf16)] * 2,
        )
        near = swap(near, "space", route.near)
        fars = [swap(far, "space", route.masks()[k]) for k, far in enumerate(fars, 2)]
        cross = call(
            functools.partial(cross_kernel, route),
            shape((2 if route.halve_phased else 1, block, width), bf16),
            0,
            1_000_000,
            (mine, near),
        )
        cross = swap(cross, "space", route.over)
        fields.extend([mine, near] + (fars or [cross]))
        sums.extend([mine, near, cross])

    strips, rounded = call(
        functools.partial(strip_kernel, plan),
        (shape((tdev, block, width), f32), shape((tdev, block, width), bf16)),
        0,
        1_000_000,
        fields,
    )
    other = swap(rounded, "tm", 1)

    rank = lax.axis_index("tm")
    global_slice = rank * tdev + jnp.arange(tdev, dtype=jnp.int32)
    target = (global_slice + jnp.take(seq_offset, global_slice)) % total_slices
    pick = (target - rank * tdev) % total_slices
    margin = call(
        functools.partial(margin_kernel, plan, scale_modes),
        shape((tdev, width), f32),
        2,
        1_000_000,
        (pick, owner_block, rounded, other, *sums),
    )
    mask = 1
    while mask < nspace:
        margin = margin + swap(margin, "space", mask)
        mask *= 2
    return jnp.transpose(strips, (1, 0, 2)), margin


def general_shards(w_modes, v_modes, phase_index, seq_offset, owner_block):
    tdev, sdev, width = w_modes.shape
    nmode = width // 2
    nspace = lax.axis_size("space")
    ntm = lax.axis_size("tm")
    block = nmode // nspace
    total_slices = tdev * ntm
    scale_sites = 1.0 / math.sqrt(sdev * nspace)
    scale_modes = 1.0 / math.sqrt(2 * nmode)
    order = (owner_block[:, None] * block + jnp.arange(block, dtype=jnp.int32)[None, :]).reshape(-1)
    w_real = jnp.take(w_modes[:, :, :nmode], order, axis=2)
    w_imag = jnp.take(w_modes[:, :, nmode:], order, axis=2)
    left = jnp.concatenate([w_real, w_imag], axis=1)
    angle = phase_index.astype(jnp.float32) * (2.0 * math.pi / PHASES)
    cosv = jnp.cos(angle)[None, :, None]
    sinv = jnp.sin(angle)[None, :, None]
    v_real = v_modes[:, :, :nmode].astype(jnp.float32)
    v_imag = v_modes[:, :, nmode:].astype(jnp.float32)
    ph_real = (cosv * v_real + sinv * v_imag).astype(jnp.bfloat16)
    ph_imag = (cosv * v_imag - sinv * v_real).astype(jnp.bfloat16)
    right = jnp.concatenate(
        [jnp.concatenate([ph_real, ph_imag], axis=2), jnp.concatenate([ph_imag, -ph_real], axis=2)],
        axis=1,
    )
    rank = lax.axis_index("tm")
    global_slice = rank * tdev + jnp.arange(tdev, dtype=jnp.int32)
    target = (global_slice + jnp.take(seq_offset, global_slice)) % total_slices
    pick = (target - rank * tdev) % total_slices
    v_two = jnp.concatenate(
        [
            jnp.concatenate([v_modes[:, :, :nmode], -v_modes[:, :, nmode:]], axis=2),
            jnp.concatenate([v_modes[:, :, nmode:], v_modes[:, :, :nmode]], axis=2),
        ],
        axis=1,
    )
    full = lax.psum(
        jnp.einsum("tsi,tsj->itj", left, right, preferred_element_type=jnp.float32) * scale_sites,
        "space",
    )
    strips = lax.dynamic_slice_in_dim(full, lax.axis_index("space") * block, block, 0)
    rounded = full.astype(jnp.bfloat16)
    pieces = [rounded]
    for step in range(1, ntm):
        route = [((i + step) % ntm, i) for i in range(ntm)]
        pieces.append(lax.ppermute(rounded, "tm", route))
    chosen = jnp.take(jnp.concatenate(pieces, axis=1), pick, axis=1)
    seq_raw = jnp.einsum("tsj,itj->tsi", v_two, chosen, preferred_element_type=jnp.float32)
    seq = seq_raw * scale_modes
    seq_real = seq[:, :sdev]
    seq_imag = seq[:, sdev:]
    wr_full = w_real.astype(jnp.float32)
    wi_full = w_imag.astype(jnp.float32)
    over_real = jnp.sum(wr_full * seq_real + wi_full * seq_imag, axis=1) * scale_sites
    over_imag = jnp.sum(wr_full * seq_imag - wi_full * seq_real, axis=1) * scale_sites
    total_real, total_imag = lax.psum((over_real, over_imag), "space")
    margin = jnp.zeros((tdev, 2 * nmode), jnp.float32)
    margin = margin.at[:, order].set(total_real).at[:, order + nmode].set(total_imag)
    return (strips, margin)


def shards(w_modes, v_modes, phase_index, seq_offset, owner_block):
    _, sdev, width = w_modes.shape
    nmode, nspace = width // 2, lax.axis_size("space")
    square = nspace == 2 * 4
    tiles = nmode % (nspace * 16) == 0 and nmode % LANES == 0 and sdev == LANES
    body = aligned_shards if square and tiles and lax.axis_size("tm") == 2 else general_shards
    return body(w_modes, v_modes, phase_index, seq_offset, owner_block)


def solution(mesh):
    in_specs = (
        P(("group", "tm"), "space", None),
        P(("group", "tm"), "space", None),
        P("space"),
        P(),
        P(),
    )
    out_specs = (P("space", ("group", "tm"), None), P(("group", "tm"), None))
    step = jax.shard_map(shards, mesh=mesh, in_specs=in_specs, out_specs=out_specs, check_vma=False)

    def run(w_modes, *rest):
        return step(w_modes, *rest)

    return run if mesh.shape["space"] == 8 else step
```
